32 devices in a mesh: band: 16 (over z, y, core), slab: 2 (over x).
Axes of the slice: x: 2, y: 2, z: 4, core: 2. Of those that a mesh axis runs over, the one named last changes fastest.
Arguments:
- orbitals: bfloat16 [32, 32, 4096], P('band', 'slab'), may hold values from -6 to 6
- occupation: bfloat16 [32], P('band'), may hold values from 0.25 to 1
Outputs:
- exchange_field: float32 [32, 32, 4096], P('band', 'slab')
The draws below stay inside these ranges and needn't reach their ends.
All inputs are finite; a program needn't handle non-finite values.
Results may differ from the reference program's by a relative error of at most 0.001.
Values may be sent and summed in bfloat16 or wider, within the bound.
A program may use at most 64 MiB of HBM per device.

```python
import math
import jax
import jax.numpy as jnp
from jax import lax

ORB_DEV = 2
NY = 64
NZ = 64
STEPS = 3
ORBITALS = 32
NX = 32
N_BAND = 16


def levels(own_key, dims, split, least, top_value):
    loudness = 1.0
    for axis_at, shards_of in split:
        steps = jax.random.uniform(jax.random.fold_in(jax.random.fold_in(own_key, 6), axis_at), (shards_of,), jnp.float32, least / len(split), top_value / len(split))
        loudness = loudness * jnp.repeat(jnp.exp(steps), dims[axis_at] // shards_of).reshape((-1,) + (1,) * (len(dims) - 1 - axis_at))
    return loudness


def centred(rng, shape, deviation, limit, shards=(), held_as=jnp.bfloat16):
    array = jax.random.normal(rng, shape, jnp.float32) * deviation
    if len(shards) > 0:
        array = levels(rng, shape, shards, -0.22, 0.18) * array
    return jnp.clip(array, min=-limit, max=limit).astype(held_as)


def setup_inputs(seed: int = 0) -> dict:
    key_list = jax.random.split(jax.random.key(seed), 3)
    return {
        "orbitals": centred(key_list[0], (ORBITALS, NX, NY * NZ), 1.0, 6.0, ((0, 16), (1, 2))),
        "occupation": jnp.clip(jnp.exp(math.log(1.0) - 1.3862944 * jax.random.uniform(key_list[1], (ORBITALS,), jnp.float32) ** levels(key_list[1], (ORBITALS,), ((0, 16),), -0.2, 0.2)), 0.25, 1.0).astype(jnp.bfloat16),
    }


screening = 0.5
ratio_mid = (12.0 + 2.0 * screening) / 12.0
root_term = math.sqrt(ratio_mid * ratio_mid - 1.0)
decay_ratio = ratio_mid - root_term
coeff_zero = 1.0 / (6.0 * root_term)
coeff_one = -2.0 * decay_ratio * coeff_zero
coeff_two = 2.0 * decay_ratio * decay_ratio * coeff_zero

def cross_sum(values):
    rest = ((0, 0),) * (values.ndim - 1)
    padded_y = jnp.pad(values, rest + ((NZ, NZ),))
    along_y = padded_y[..., 2 * NZ:] + padded_y[..., :-2 * NZ]
    narrow = jnp.pad(values, rest + ((1, 1),))
    column = jnp.arange(values.shape[-1], dtype=jnp.int32) % NZ
    left_side = jnp.where(column != 0, narrow[..., :-2], 0.0)
    right_side = jnp.where(column != NZ - 1, narrow[..., 2:], 0.0)
    return along_y + (left_side + right_side)

def neighbour(values):
    padded = jnp.pad(values, ((0, 0), (0, 0), (1, 1), (0, 0)))
    return padded[:, :, 2:] + padded[:, :, :-2] + cross_sum(values)

def reference(orbitals, occupation):
    cells = NY * NZ
    orbital_grid = orbitals.astype(jnp.float32).reshape(N_BAND, ORB_DEV, NX, cells)
    occupied = occupation.astype(jnp.float32).reshape(N_BAND, ORB_DEV)

    def one_block(block_index):
        own_block = lax.dynamic_index_in_dim(orbital_grid, block_index, 0, keepdims=False)
        running = jnp.zeros((ORB_DEV, NX, cells), jnp.float32)
        for visit in range(STEPS + 1):
            source_block = ((block_index - visit) % N_BAND).astype(jnp.int32)
            visitor = lax.dynamic_index_in_dim(orbital_grid, source_block, 0, keepdims=False)
            weights = lax.dynamic_index_in_dim(occupied, source_block, 0, keepdims=False)
            density = own_block[:, None] * visitor[None]
            first_term = -neighbour(density) / 6.0
            second_term = -neighbour(first_term) / 3.0 - density
            potential = coeff_zero * density + coeff_one * first_term + coeff_two * second_term
            running = running - lax.optimization_barrier(jnp.sum(weights[None, :, None, None] * visitor[None] * potential, axis=1))
        return running
    result = lax.map(one_block, jnp.arange(N_BAND, dtype=jnp.int32))
    return result.reshape(ORBITALS, NX, cells)
```

```python
import functools
import math

import jax
import jax.numpy as jnp
from jax import lax
from jax.experimental import pallas as pl
from jax.experimental.pallas import tpu as pltpu
from jax.sharding import PartitionSpec as P

NZ = 64
STEPS = 3
LANES = 128
WIDTH = 2
UNROLL = 4
MESH = pl.DeviceIdType.MESH


screening = 0.5
ratio_mid = (12.0 + 2.0 * screening) / 12.0
root_term = math.sqrt(ratio_mid * ratio_mid - 1.0)
decay_ratio = ratio_mid - root_term
coeff_zero = 1.0 / (6.0 * root_term)
coeff_one = -2.0 * decay_ratio * coeff_zero
coeff_two = 2.0 * decay_ratio * decay_ratio * coeff_zero

scale = coeff_two / 18.0
inner = -coeff_one / 6.0 / scale
outer = (coeff_zero - coeff_two) / scale


def loop(count, body, unroll=1):
    lax.fori_loop(0, count, lambda i, c: (body(i), c)[1], 0, unroll=unroll)


def lane_tile(t):
    return pl.ds(pl.multiple_of(t * LANES, LANES), LANES)


def kernel(n_band, n_slab, orb_ref, occ_ref, out_ref, block, slots, edges, halos, own, vis,
           weighted, dens, inner_field, load_sem, send_sem, recv_sem, edge_send, edge_recv):
    orbs, planes, cells = orb_ref.shape
    tiles = cells // LANES
    ext = vis.shape[2]
    band, slab = lax.axis_index("band"), lax.axis_index("slab")
    odd = lax.rem(band, 2)

    def at(by, side=0):
        return {"band": lax.rem(band + by + n_band, n_band), "slab": slab + side}

    sibling = at(1 - 2 * odd)
    has = (slab > 0, slab < n_slab - 1)
    step_of = (-1, 1)

    load = pltpu.make_async_copy(orb_ref, block.at[:, :, :cells], load_sem.at[0])
    load_occ = pltpu.make_async_copy(occ_ref, block.at[:, :, cells:], load_sem.at[1])
    load.start()
    load_occ.start()

    barrier = pltpu.get_barrier_semaphore()
    pl.semaphore_signal(barrier, inc=1, device_id=at(-2), device_id_type=MESH)
    pl.semaphore_signal(barrier, inc=1, device_id=at(2 * odd - 3), device_id_type=MESH)
    pl.semaphore_signal(barrier, inc=1, device_id=sibling, device_id_type=MESH)
    for side in range(2):
        @pl.when(has[side])
        def _(side=side):
            for s in range(STEPS + 1):
                pl.semaphore_signal(barrier, inc=1, device_id=at(-s, step_of[side]), device_id_type=MESH)

    load.wait()
    load_occ.wait()

    def cut(k):
        parts = ([], [])
        for h in range(2):
            for o in range(orbs):
                tile = block[o, :, lane_tile(2 * k + h)].astype(jnp.float32)
                parts[0].append(tile[:WIDTH])
                parts[1].append(tile[planes - WIDTH:])
        for side in range(2):
            edges[side, k] = jnp.concatenate(parts[side], axis=0).astype(jnp.bfloat16)

    loop(tiles // 2, cut, 2)

    for side in range(2):
        @pl.when(jnp.logical_not(has[side]))
        def _(side=side):
            halos[:, side] = jnp.zeros(halos.shape[:1] + halos.shape[2:], jnp.bfloat16)

    sides = has[0].astype(jnp.int32) + has[1].astype(jnp.int32)
    pl.semaphore_wait(barrier, 3 + (STEPS + 1) * sides)

    def edge_copy(side, s):
        return pltpu.make_async_remote_copy(
            src_ref=edges.at[side], dst_ref=halos.at[s, 1 - side],
            send_sem=edge_send.at[s, side], recv_sem=edge_recv.at[s, 1 - side],
            device_id=at(s, step_of[side]), device_id_type=MESH)

    def edge_wait(side, s):
        return pltpu.make_async_remote_copy(
            src_ref=edges.at[1 - side], dst_ref=halos.at[s, side],
            send_sem=edge_send.at[s, 1 - side], recv_sem=edge_recv.at[s, side],
            device_id=at(s, step_of[side]), device_id_type=MESH)

    def block_copy(src, slot, to):
        return pltpu.make_async_remote_copy(
            src_ref=src, dst_ref=slots.at[slot], send_sem=send_sem.at[slot],
            recv_sem=recv_sem.at[slot], device_id=to, device_id_type=MESH)

    def send_edges(steps):
        for side in range(2):
            @pl.when(has[side])
            def _(side=side):
                for s in steps:
                    edge_copy(side, s).start()

    direct = block_copy(block, 0, at(1 + 2 * odd))
    second = block_copy(block, 1, at(2))
    passed = block_copy(slots.at[1], 2, sibling)
    send_edges((0,))
    second.start()
    direct.start()
    send_edges(range(1, STEPS + 1))

    for p in range(orbs * orbs):
        for t in (0, tiles + 1):
            dens[p, t] = jnp.zeros(dens.shape[2:], jnp.float32)
            inner_field[p, t] = jnp.zeros(inner_field.shape[2:], jnp.float32)

    lane = lax.broadcasted_iota(jnp.int32, (1, LANES), 1)
    high = lane >= NZ
    column = lane % NZ
    first_col, last_col = column == 0, column == NZ - 1
    row = lax.broadcasted_iota(jnp.int32, (ext, LANES), 0)
    below = jnp.where(has[0], 1.0, 0.0)
    above = jnp.where(has[1], 1.0, 0.0)
    row_mask = jnp.where(row == 0, below, jnp.where(row == planes + 1, above, 1.0))

    def across(mid, before, after):
        pairs = pltpu.roll(mid + jnp.where(high, before, after), NZ, 1)
        left = pltpu.roll(jnp.where(last_col, 0.0, mid), 1, 1)
        right = pltpu.roll(jnp.where(first_col, 0.0, mid), LANES - 1, 1)
        return pairs + (left + right)

    def widen(src, low, up, dst):
        def body(k):
            lo = low[k].astype(jnp.float32)
            hi = up[k].astype(jnp.float32)
            for h in range(2):
                for o in range(orbs):
                    t = 2 * k + h
                    r = (h * orbs + o) * WIDTH
                    dst[o, t, :WIDTH] = lo[r:r + WIDTH]
                    dst[o, t, planes + WIDTH:planes + 2 * WIDTH] = hi[r:r + WIDTH]
                    dst[o, t, WIDTH:planes + WIDTH] = src[o, :, lane_tile(t)].astype(jnp.float32)
        loop(tiles // 2, body, 2)

    def visit(src, other, first):
        weights = [-scale * src[o, :, cells:].astype(jnp.float32) for o in range(orbs)]

        def density(t):
            for o in range(orbs):
                weighted[o, t] = weights[o] * other[o, t, WIDTH:planes + WIDTH]
            for i in range(orbs):
                for j in range(orbs):
                    dens[i * orbs + j, t + 1, :ext] = own[i, t] * other[j, t]

        def once(t):
            for p in range(orbs * orbs):
                mid = dens[p, t + 1, 1:ext + 1]
                along = dens[p, t + 1, :ext] + dens[p, t + 1, 2:ext + 2]
                u = inner * mid + along + across(mid, dens[p, t, 1:ext + 1], dens[p, t + 2, 1:ext + 1])
                inner_field[p, t + 1] = u * row_mask

        def twice(t):
            for i in range(orbs):
                total = None
                for j in range(orbs):
                    p = i * orbs + j
                    mid = inner_field[p, t + 1, 1:planes + 1]
                    along = inner_field[p, t + 1, :planes] + inner_field[p, t + 1, 2:planes + 2]
                    v = along + across(mid, inner_field[p, t, 1:planes + 1], inner_field[p, t + 2, 1:planes + 1])
                    v = v + outer * dens[p, t + 1, WIDTH:planes + WIDTH]
                    term = weighted[j, t] * v
                    total = term if total is None else total + term
                if not first:
                    total = total + out_ref[i, :, lane_tile(t)]
                out_ref[i, :, lane_tile(t)] = total

        loop(tiles, density, UNROLL)
        loop(tiles, once, UNROLL)
        loop(tiles, twice, UNROLL)

    def wait_halos(s):
        for side in range(2):
            @pl.when(has[side])
            def _(side=side):
                edge_wait(side, s).wait_recv()

    wait_halos(0)
    widen(block, halos.at[0, 0], halos.at[0, 1], own)
    visit(block, own, True)

    second.wait_recv()
    passed.start()
    wait_halos(2)
    widen(slots.at[1], halos.at[2, 0], halos.at[2, 1], vis)
    visit(slots.at[1], vis, False)

    wait_halos(1)
    wait_halos(3)
    for slot, wait, step in ((0, direct, 3 - 2 * odd), (2, passed, 1 + 2 * odd)):
        wait.wait_recv()
        widen(slots.at[slot], halos.at[step, 0], halos.at[step, 1], vis)
        visit(slots.at[slot], vis, False)

    direct.wait_send()
    second.wait_send()
    passed.wait_send()
    for side in range(2):
        @pl.when(has[side])
        def _(side=side):
            for s in range(STEPS + 1):
                edge_copy(side, s).wait_send()


def per_device(n_band, n_slab, orbitals, occupation):
    orbs, planes, cells = orbitals.shape
    tiles = cells // LANES
    ext = -(-(planes + 2 * WIDTH) // 8) * 8
    occ = jnp.broadcast_to(occupation[:, None, None], (orbs, planes, LANES))
    f32, bf16 = jnp.float32, jnp.bfloat16
    rows = 2 * orbs * WIDTH
    return pl.pallas_call(
        functools.partial(kernel, n_band, n_slab),
        out_shape=jax.ShapeDtypeStruct(orbitals.shape, f32),
        in_specs=[pl.BlockSpec(memory_space=pl.ANY)] * 2,
        out_specs=pl.BlockSpec(memory_space=pltpu.VMEM),
        scratch_shapes=[
            pltpu.VMEM((orbs, planes, cells + LANES), bf16),
            pltpu.VMEM((STEPS, orbs, planes, cells + LANES), bf16),
            pltpu.VMEM((2, tiles // 2, rows, LANES), bf16),
            pltpu.VMEM((STEPS + 1, 2, tiles // 2, rows, LANES), bf16),
            pltpu.VMEM((orbs, tiles, ext, LANES), f32),
            pltpu.VMEM((orbs, tiles, ext, LANES), f32),
            pltpu.VMEM((orbs, tiles, planes, LANES), f32),
            pltpu.VMEM((orbs * orbs, tiles + 2, ext + 8, LANES), f32),
            pltpu.VMEM((orbs * orbs, tiles + 2, ext, LANES), f32),
            pltpu.SemaphoreType.DMA((2,)),
            pltpu.SemaphoreType.DMA((STEPS,)),
            pltpu.SemaphoreType.DMA((STEPS,)),
            pltpu.SemaphoreType.DMA((STEPS + 1, 2)),
            pltpu.SemaphoreType.DMA((STEPS + 1, 2)),
        ],
        compiler_params=pltpu.CompilerParams(collective_id=0, has_side_effects=True),
        name="exchange",
    )(orbitals, occ)


def solution(mesh):
    in_specs = (P("band", "slab", None), P("band"))
    out_specs = P("band", "slab", None)
    return jax.shard_map(
        functools.partial(per_device, mesh.shape["band"], mesh.shape["slab"]),
        mesh=mesh, in_specs=in_specs, out_specs=out_specs, check_vma=False,
    )
```

```python
import functools
import math

import jax
import jax.numpy as jnp
from jax import lax
from jax.experimental import pallas as pl
from jax.experimental.pallas import tpu as pltpu
from jax.sharding import PartitionSpec as P

NZ = 64
STEPS = 3
LANES = 128
WIDTH = 2
UNROLL = 4
MESH = pl.DeviceIdType.MESH


screening = 0.5
ratio_mid = (12.0 + 2.0 * screening) / 12.0
root_term = math.sqrt(ratio_mid * ratio_mid - 1.0)
decay_ratio = ratio_mid - root_term
coeff_zero = 1.0 / (6.0 * root_term)
coeff_one = -2.0 * decay_ratio * coeff_zero
coeff_two = 2.0 * decay_ratio * decay_ratio * coeff_zero

scale = coeff_two / 18.0
inner = -coeff_one / 6.0 / scale
outer = (coeff_zero - coeff_two) / scale


def loop(count, body, unroll=1):
    lax.fori_loop(0, count, lambda i, c: (body(i), c)[1], 0, unroll=unroll)


def lane_tile(t):
    return pl.ds(pl.multiple_of(t * LANES, LANES), LANES)


def kernel(n_band, n_slab, orb_ref, occ_ref, out_ref, slots, edges, halos, own, own_moved, vis,
           weighted, dens, turned, part, inner_field, load_sem, send_sem, recv_sem, edge_send, edge_recv):
    orbs, planes, cells = orb_ref.shape
    tiles = cells // LANES
    ext = vis.shape[1]
    mine = STEPS
    band, slab = lax.axis_index("band"), lax.axis_index("slab")
    odd = lax.rem(band, 2)

    def at(by, side=0):
        return {"band": lax.rem(band + by + n_band, n_band), "slab": slab + side}

    sibling = at(1 - 2 * odd)
    has = (slab > 0, slab < n_slab - 1)
    step_of = (-1, 1)
    reach = {mine: 0, 1: 2, 0: 1 + 2 * odd}
    source = {mine: 0, 1: -2, 0: 2 * odd - 3}

    load = pltpu.make_async_copy(orb_ref, slots.at[mine, :, :, :cells], load_sem.at[0])
    load_occ = pltpu.make_async_copy(occ_ref, slots.at[mine, :, :, cells:], load_sem.at[1])
    load.start()
    load_occ.start()

    barrier = pltpu.get_barrier_semaphore()
    for by in (source[1], source[0]):
        pl.semaphore_signal(barrier, inc=1, device_id=at(by), device_id_type=MESH)
    pl.semaphore_signal(barrier, inc=1, device_id=sibling, device_id_type=MESH)
    for side in range(2):
        @pl.when(has[side])
        def _(side=side):
            for slot in (mine, 1, 0):
                pl.semaphore_signal(barrier, inc=1, device_id=at(source[slot], step_of[side]), device_id_type=MESH)

    load.wait()
    load_occ.wait()

    def cut(k):
        parts = ([], [])
        for h in range(2):
            for o in range(orbs):
                tile = slots[mine, o, :, lane_tile(2 * k + h)].astype(jnp.float32)
                parts[0].append(tile[:WIDTH])
                parts[1].append(tile[planes - WIDTH:])
        for side in range(2):
            edges[side, k] = jnp.concatenate(parts[side], axis=0).astype(jnp.bfloat16)

    loop(tiles // 2, cut, 2)

    for side in range(2):
        @pl.when(jnp.logical_not(has[side]))
        def _(side=side):
            halos[:, side] = jnp.zeros(halos.shape[:1] + halos.shape[2:], jnp.bfloat16)

    sides = has[0].astype(jnp.int32) + has[1].astype(jnp.int32)
    pl.semaphore_wait(barrier, 3 + 3 * sides)

    def edge_copy(side, slot):
        return pltpu.make_async_remote_copy(
            src_ref=edges.at[side], dst_ref=halos.at[slot, 1 - side],
            send_sem=edge_send.at[slot, side], recv_sem=edge_recv.at[slot, 1 - side],
            device_id=at(reach[slot], step_of[side]), device_id_type=MESH)

    def edge_pass(side):
        return pltpu.make_async_remote_copy(
            src_ref=halos.at[1, side], dst_ref=halos.at[2, side],
            send_sem=edge_send.at[2, side], recv_sem=edge_recv.at[2, side],
            device_id=sibling, device_id_type=MESH)

    def edge_wait(side, slot):
        pltpu.make_async_remote_copy(
            src_ref=edges.at[1 - side], dst_ref=halos.at[slot, side],
            send_sem=edge_send.at[slot, 1 - side], recv_sem=edge_recv.at[slot, side],
            device_id=sibling, device_id_type=MESH).wait_recv()

    def block_copy(slot, o):
        return pltpu.make_async_remote_copy(
            src_ref=slots.at[mine, o], dst_ref=slots.at[slot, o], send_sem=send_sem.at[slot, o],
            recv_sem=recv_sem.at[slot, o], device_id=at(reach[slot]), device_id_type=MESH)

    def block_pass(o):
        return pltpu.make_async_remote_copy(
            src_ref=slots.at[1, o], dst_ref=slots.at[2, o], send_sem=send_sem.at[2, o],
            recv_sem=recv_sem.at[2, o], device_id=sibling, device_id_type=MESH)

    def each_side(action):
        for side in range(2):
            pl.when(has[side])(functools.partial(action, side))

    each_side(lambda side: edge_copy(side, mine).start())
    each_side(lambda side: edge_copy(side, 1).start())
    each_side(lambda side: edge_copy(side, 0).start())
    for o in range(orbs):
        block_copy(1, o).start()
        block_copy(0, o).start()

    for i in range(orbs):
        for t in (0, tiles + 1):
            turned[i, t] = jnp.zeros(turned.shape[2:], jnp.float32)
            inner_field[i, t] = jnp.zeros(inner_field.shape[2:], jnp.float32)

    lane = lax.broadcasted_iota(jnp.int32, (1, LANES), 1)
    high = lane >= NZ
    column = lane % NZ
    first_col, last_col = column == 0, column == NZ - 1
    row = lax.broadcasted_iota(jnp.int32, (ext, LANES), 0)
    below = jnp.where(has[0], 1.0, 0.0)
    above = jnp.where(has[1], 1.0, 0.0)
    row_mask = jnp.where(row == WIDTH - 1, below, jnp.where(row == planes + WIDTH, above, 1.0))

    def from_left(mid):
        return pltpu.roll(jnp.where(last_col, 0.0, mid), 1, 1)

    def from_right(mid):
        return pltpu.roll(jnp.where(first_col, 0.0, mid), LANES - 1, 1)

    def widen(slot, o, dst):
        def body(k):
            low = halos[slot, 0, k].astype(jnp.float32)
            up = halos[slot, 1, k].astype(jnp.float32)
            for h in range(2):
                t = 2 * k + h
                for q in range(orbs):
                    @pl.when(o == q)
                    def _(q=q, h=h, t=t):
                        r = (h * orbs + q) * WIDTH
                        dst[t, :WIDTH] = low[r:r + WIDTH]
                        dst[t, planes + WIDTH:planes + 2 * WIDTH] = up[r:r + WIDTH]
                dst[t, WIDTH:planes + WIDTH] = slots[slot, o, :, lane_tile(t)].astype(jnp.float32)
        loop(tiles // 2, body, 2)

    def visit(slot, o):
        weight = -scale * slots[slot, o, :, cells:].astype(jnp.float32)
        widen(slot, o, vis)

        def density(t):
            mid = vis[t]
            moved = (pltpu.roll(mid, NZ, 1), from_left(mid), from_right(mid))
            weighted[t] = weight * vis[t, WIDTH:planes + WIDTH]
            for i in range(orbs):
                d = own[i, t] * mid
                dens[i, t, 8:ext + 8] = d
                turn = own_moved[i, 0, t] * moved[0]
                turned[i, t + 1] = turn
                part[i, t] = inner * d + turn + (own_moved[i, 1, t] * moved[1] + own_moved[i, 2, t] * moved[2])

        def once(t):
            for i in range(orbs):
                along = dens[i, t, 7:ext + 7] + dens[i, t, 9:ext + 9]
                u = part[i, t] + along + jnp.where(high, turned[i, t + 2], turned[i, t])
                inner_field[i, t + 1] = u * row_mask

        def twice(t):
            for i in range(orbs):
                mid = inner_field[i, t + 1, WIDTH:planes + WIDTH]
                before = inner_field[i, t, WIDTH:planes + WIDTH]
                after = inner_field[i, t + 2, WIDTH:planes + WIDTH]
                v = inner_field[i, t + 1, WIDTH - 1:planes + WIDTH - 1] + inner_field[i, t + 1, WIDTH + 1:planes + WIDTH + 1]
                v = v + pltpu.roll(mid + jnp.where(high, before, after), NZ, 1)
                v = v + (from_left(mid) + from_right(mid))
                v = v + outer * dens[i, t, 8 + WIDTH:8 + planes + WIDTH]
                out_ref[i, :, lane_tile(t)] += weighted[t] * v

        loop(tiles, density, UNROLL)
        loop(tiles, once, UNROLL)
        loop(tiles, twice, UNROLL)

    each_side(lambda side: edge_wait(side, mine))
    for i in range(orbs):
        widen(mine, i, own.at[i])

    def prepare(t):
        for i in range(orbs):
            mid = own[i, t]
            own_moved[i, 0, t] = pltpu.roll(mid, NZ, 1)
            own_moved[i, 1, t] = from_left(mid)
            own_moved[i, 2, t] = from_right(mid)
            out_ref[i, :, lane_tile(t)] = jnp.zeros((planes, LANES), jnp.float32)

    loop(tiles, prepare, UNROLL)

    if_odd, if_even = [(mine, o) for o in range(orbs)], [(mine, o) for o in range(orbs)]
    if_odd += [(0, o) for o in range(orbs)]
    for o in range(orbs):
        if_odd += [(1, o), (2, o)]
        if_even += [(1, o), (0, o), (2, o)]

    def entry(k, column):
        value = jnp.int32(0)
        for n, (a, b) in enumerate(zip(if_odd, if_even)):
            value = jnp.where(k == n, jnp.where(odd == 1, a[column], b[column]), value)
        return value

    def step(k):
        slot, o = entry(k, 0), entry(k, 1)
        for q in range(STEPS):
            for p in range(orbs):
                @pl.when(jnp.logical_and(slot == q, o == p))
                def _(q=q, p=p):
                    if p == 0:
                        each_side(lambda side: edge_wait(side, q))
                        if q == 1:
                            each_side(lambda side: edge_pass(side).start())
                    (block_pass(p) if q == 2 else block_copy(q, p)).wait_recv()
                    if q == 1:
                        block_pass(p).start()
        visit(slot, o)

    loop(len(if_odd), step)

    for o in range(orbs):
        block_copy(0, o).wait_send()
        block_copy(1, o).wait_send()
        block_pass(o).wait_send()
    for slot in (mine, 1, 0):
        each_side(lambda side: edge_copy(side, slot).wait_send())
    each_side(lambda side: edge_pass(side).wait_send())


def per_device(n_band, n_slab, orbitals, occupation):
    orbs, planes, cells = orbitals.shape
    tiles = cells // LANES
    ext = -(-(planes + 2 * WIDTH) // 8) * 8
    occ = jnp.broadcast_to(occupation[:, None, None], (orbs, planes, LANES))
    f32, bf16 = jnp.float32, jnp.bfloat16
    rows = 2 * orbs * WIDTH
    return pl.pallas_call(
        functools.partial(kernel, n_band, n_slab),
        out_shape=jax.ShapeDtypeStruct(orbitals.shape, f32),
        in_specs=[pl.BlockSpec(memory_space=pl.ANY)] * 2,
        out_specs=pl.BlockSpec(memory_space=pltpu.VMEM),
        scratch_shapes=[
            pltpu.VMEM((STEPS + 1, orbs, planes, cells + LANES), bf16),
            pltpu.VMEM((2, tiles // 2, rows, LANES), bf16),
            pltpu.VMEM((STEPS + 1, 2, tiles // 2, rows, LANES), bf16),
            pltpu.VMEM((orbs, tiles, ext, LANES), f32),
            pltpu.VMEM((orbs, 3, tiles, ext, LANES), f32),
            pltpu.VMEM((tiles, ext, LANES), f32),
            pltpu.VMEM((tiles, planes, LANES), f32),
            pltpu.VMEM((orbs, tiles, ext + 16, LANES), f32),
            pltpu.VMEM((orbs, tiles + 2, ext, LANES), f32),
            pltpu.VMEM((orbs, tiles, ext, LANES), f32),
            pltpu.VMEM((orbs, tiles + 2, ext, LANES), f32),
            pltpu.SemaphoreType.DMA((2,)),
            pltpu.SemaphoreType.DMA((STEPS, orbs)),
            pltpu.SemaphoreType.DMA((STEPS, orbs)),
            pltpu.SemaphoreType.DMA((STEPS + 1, 2)),
            pltpu.SemaphoreType.DMA((STEPS + 1, 2)),
        ],
        compiler_params=pltpu.CompilerParams(collective_id=0, has_side_effects=True),
        name="exchange",
    )(orbitals, occ)


def solution(mesh):
    in_specs = (P("band", "slab", None), P("band"))
    out_specs = P("band", "slab", None)
    return jax.shard_map(
        functools.partial(per_device, mesh.shape["band"], mesh.shape["slab"]),
        mesh=mesh, in_specs=in_specs, out_specs=out_specs, check_vma=False,
    )
```

```python
import functools
import math

import jax
import jax.numpy as jnp
from jax import lax
from jax.experimental import pallas as pl
from jax.experimental.pallas import tpu as pltpu
from jax.sharding import PartitionSpec as P

NZ = 64
STEPS = 3
LANES = 128
WIDTH = 2
UNROLL = 8
MESH = pl.DeviceIdType.MESH


screening = 0.5
ratio_mid = (12.0 + 2.0 * screening) / 12.0
root_term = math.sqrt(ratio_mid * ratio_mid - 1.0)
decay_ratio = ratio_mid - root_term
coeff_zero = 1.0 / (6.0 * root_term)
coeff_one = -2.0 * decay_ratio * coeff_zero
coeff_two = 2.0 * decay_ratio * decay_ratio * coeff_zero

scale = coeff_two / 18.0
inner = -coeff_one / 6.0 / scale
outer = (coeff_zero - coeff_two) / scale


def loop(count, body, unroll=1):
    lax.fori_loop(0, count, lambda i, c: (body(i), c)[1], 0, unroll=unroll)


def lane_tile(t):
    return pl.ds(pl.multiple_of(t * LANES, LANES), LANES)


def kernel(n_band, n_slab, orb_ref, occ_ref, out_ref, slots, edges, halos, own, own_moved, vis,
           weighted, dens, turned, part, inner_field, load_sem, send_sem, recv_sem, edge_send, edge_recv):
    orbs, planes, cells = orb_ref.shape
    tiles = cells // LANES
    ext = vis.shape[1]
    mine = STEPS
    band, slab = lax.axis_index("band"), lax.axis_index("slab")
    odd = lax.rem(band, 2)

    def at(by, side=0):
        return {"band": lax.rem(band + by + n_band, n_band), "slab": slab + side}

    sibling = at(1 - 2 * odd)
    has = (slab > 0, slab < n_slab - 1)
    step_of = (-1, 1)
    reach = {mine: 0, 1: 2, 0: 1 + 2 * odd}
    source = {mine: 0, 1: -2, 0: 2 * odd - 3}

    load = pltpu.make_async_copy(orb_ref, slots.at[mine, :, :, :cells], load_sem.at[0])
    load.start()

    barrier = pltpu.get_barrier_semaphore()
    for by in (source[1], source[0]):
        pl.semaphore_signal(barrier, inc=1, device_id=at(by), device_id_type=MESH)
    pl.semaphore_signal(barrier, inc=1, device_id=sibling, device_id_type=MESH)
    for side in range(2):
        @pl.when(has[side])
        def _(side=side):
            for slot in (mine, 1, 0):
                pl.semaphore_signal(barrier, inc=1, device_id=at(source[slot], step_of[side]), device_id_type=MESH)

    load.wait()
    for o in range(orbs):
        value = jnp.broadcast_to(occ_ref[:, o:o + 1].astype(jnp.float32), (planes, LANES))
        slots[mine, o, :, cells:] = value.astype(jnp.bfloat16)

    def cut(k):
        parts = ([], [])
        for h in range(2):
            for o in range(orbs):
                tile = slots[mine, o, :, lane_tile(2 * k + h)].astype(jnp.float32)
                parts[0].append(tile[:WIDTH])
                parts[1].append(tile[planes - WIDTH:])
        for side in range(2):
            edges[side, k] = jnp.concatenate(parts[side], axis=0).astype(jnp.bfloat16)

    loop(tiles // 2, cut, 2)

    for side in range(2):
        @pl.when(jnp.logical_not(has[side]))
        def _(side=side):
            halos[:, side] = jnp.zeros(halos.shape[:1] + halos.shape[2:], jnp.bfloat16)

    sides = has[0].astype(jnp.int32) + has[1].astype(jnp.int32)
    pl.semaphore_wait(barrier, 3 + 3 * sides)

    def edge_copy(side, slot):
        return pltpu.make_async_remote_copy(
            src_ref=edges.at[side], dst_ref=halos.at[slot, 1 - side],
            send_sem=edge_send.at[slot, side], recv_sem=edge_recv.at[slot, 1 - side],
            device_id=at(reach[slot], step_of[side]), device_id_type=MESH)

    def edge_pass(side):
        return pltpu.make_async_remote_copy(
            src_ref=halos.at[1, side], dst_ref=halos.at[2, side],
            send_sem=edge_send.at[2, side], recv_sem=edge_recv.at[2, side],
            device_id=sibling, device_id_type=MESH)

    def edge_wait(side, slot):
        pltpu.make_async_remote_copy(
            src_ref=edges.at[1 - side], dst_ref=halos.at[slot, side],
            send_sem=edge_send.at[slot, 1 - side], recv_sem=edge_recv.at[slot, side],
            device_id=sibling, device_id_type=MESH).wait_recv()

    def block_copy(slot, o):
        return pltpu.make_async_remote_copy(
            src_ref=slots.at[mine, o], dst_ref=slots.at[slot, o], send_sem=send_sem.at[slot, o],
            recv_sem=recv_sem.at[slot, o], device_id=at(reach[slot]), device_id_type=MESH)

    def block_pass(o):
        return pltpu.make_async_remote_copy(
            src_ref=slots.at[1, o], dst_ref=slots.at[2, o], send_sem=send_sem.at[2, o],
            recv_sem=recv_sem.at[2, o], device_id=sibling, device_id_type=MESH)

    def each_side(action):
        for side in range(2):
            pl.when(has[side])(functools.partial(action, side))

    each_side(lambda side: edge_copy(side, mine).start())
    each_side(lambda side: edge_copy(side, 1).start())
    each_side(lambda side: edge_copy(side, 0).start())
    for o in range(orbs):
        block_copy(1, o).start()
        block_copy(0, o).start()

    for i in range(orbs):
        for t in (0, tiles + 1):
            turned[i, t] = jnp.zeros(turned.shape[2:], jnp.float32)
            inner_field[i, t] = jnp.zeros(inner_field.shape[2:], jnp.float32)

    lane = lax.broadcasted_iota(jnp.int32, (1, LANES), 1)
    high = lane >= NZ
    column = lane % NZ
    first_col, last_col = column == 0, column == NZ - 1
    row = lax.broadcasted_iota(jnp.int32, (ext, LANES), 0)
    below = jnp.where(has[0], 1.0, 0.0)
    above = jnp.where(has[1], 1.0, 0.0)
    row_mask = jnp.where(row == WIDTH - 1, below, jnp.where(row == planes + WIDTH, above, 1.0))

    def from_left(mid):
        return pltpu.roll(jnp.where(last_col, 0.0, mid), 1, 1)

    def from_right(mid):
        return pltpu.roll(jnp.where(first_col, 0.0, mid), LANES - 1, 1)

    def pick(rows, h, o):
        value = None
        for q in range(orbs):
            r = (h * orbs + q) * WIDTH
            piece = rows[r:r + WIDTH]
            value = piece if value is None else jnp.where(o == q, piece, value)
        return value

    def widen(slot, o, dst):
        def body(k):
            low = halos[slot, 0, k].astype(jnp.float32)
            up = halos[slot, 1, k].astype(jnp.float32)
            for h in range(2):
                t = 2 * k + h
                dst[t, :WIDTH] = pick(low, h, o)
                dst[t, planes + WIDTH:planes + 2 * WIDTH] = pick(up, h, o)
                dst[t, WIDTH:planes + WIDTH] = slots[slot, o, :, lane_tile(t)].astype(jnp.float32)
        loop(tiles // 2, body, 4)

    def visit(slot, o):
        weight = -scale * slots[slot, o, :, cells:].astype(jnp.float32)
        widen(slot, o, vis)

        def density(t):
            mid = vis[t]
            moved = (pltpu.roll(mid, NZ, 1), from_left(mid), from_right(mid))
            weighted[t] = weight * vis[t, WIDTH:planes + WIDTH]
            for i in range(orbs):
                d = own[i, t] * mid
                dens[i, t, 8:ext + 8] = d
                turn = own_moved[i, 0, t] * moved[0]
                turned[i, t + 1] = turn
                part[i, t] = inner * d + turn + (own_moved[i, 1, t] * moved[1] + own_moved[i, 2, t] * moved[2])

        def once(t):
            for i in range(orbs):
                along = dens[i, t, 7:ext + 7] + dens[i, t, 9:ext + 9]
                u = part[i, t] + along + jnp.where(high, turned[i, t + 2], turned[i, t])
                inner_field[i, t + 1] = u * row_mask

        def twice(t):
            for i in range(orbs):
                mid = inner_field[i, t + 1, WIDTH:planes + WIDTH]
                before = inner_field[i, t, WIDTH:planes + WIDTH]
                after = inner_field[i, t + 2, WIDTH:planes + WIDTH]
                v = inner_field[i, t + 1, WIDTH - 1:planes + WIDTH - 1] + inner_field[i, t + 1, WIDTH + 1:planes + WIDTH + 1]
                v = v + pltpu.roll(mid + jnp.where(high, before, after), NZ, 1)
                v = v + (from_left(mid) + from_right(mid))
                v = v + outer * dens[i, t, 8 + WIDTH:8 + planes + WIDTH]
                out_ref[i, :, lane_tile(t)] += weighted[t] * v

        loop(tiles, density, UNROLL)
        loop(tiles, once, UNROLL)
        loop(tiles, twice, UNROLL)

    each_side(lambda side: edge_wait(side, mine))
    for i in range(orbs):
        widen(mine, i, own.at[i])

    def prepare(t):
        for i in range(orbs):
            mid = own[i, t]
            own_moved[i, 0, t] = pltpu.roll(mid, NZ, 1)
            own_moved[i, 1, t] = from_left(mid)
            own_moved[i, 2, t] = from_right(mid)
            out_ref[i, :, lane_tile(t)] = jnp.zeros((planes, LANES), jnp.float32)

    loop(tiles, prepare, UNROLL)

    if_odd, if_even = [(mine, o) for o in range(orbs)], [(mine, o) for o in range(orbs)]
    if_odd += [(0, o) for o in range(orbs)]
    for o in range(orbs):
        if_odd += [(1, o), (2, o)]
        if_even += [(1, o), (0, o), (2, o)]

    def entry(k, column):
        value = jnp.int32(0)
        for n, (a, b) in enumerate(zip(if_odd, if_even)):
            value = jnp.where(k == n, jnp.where(odd == 1, a[column], b[column]), value)
        return value

    def step(k):
        slot, o = entry(k, 0), entry(k, 1)
        for q in range(STEPS):
            for p in range(orbs):
                @pl.when(jnp.logical_and(slot == q, o == p))
                def _(q=q, p=p):
                    if p == 0:
                        each_side(lambda side: edge_wait(side, q))
                        if q == 1:
                            each_side(lambda side: edge_pass(side).start())
                    (block_pass(p) if q == 2 else block_copy(q, p)).wait_recv()
                    if q == 1:
                        block_pass(p).start()
        visit(slot, o)

    loop(len(if_odd), step)

    for o in range(orbs):
        block_copy(0, o).wait_send()
        block_copy(1, o).wait_send()
        block_pass(o).wait_send()
    for slot in (mine, 1, 0):
        each_side(lambda side: edge_copy(side, slot).wait_send())
    each_side(lambda side: edge_pass(side).wait_send())


def per_device(n_band, n_slab, orbitals, occupation):
    orbs, planes, cells = orbitals.shape
    tiles = cells // LANES
    ext = -(-(planes + 2 * WIDTH) // 8) * 8
    occ = occupation.reshape(1, orbs)
    f32, bf16 = jnp.float32, jnp.bfloat16
    rows = 2 * orbs * WIDTH
    return pl.pallas_call(
        functools.partial(kernel, n_band, n_slab),
        out_shape=jax.ShapeDtypeStruct(orbitals.shape, f32),
        in_specs=[pl.BlockSpec(memory_space=pl.ANY), pl.BlockSpec(memory_space=pltpu.VMEM)],
        out_specs=pl.BlockSpec(memory_space=pltpu.VMEM),
        scratch_shapes=[
            pltpu.VMEM((STEPS + 1, orbs, planes, cells + LANES), bf16),
            pltpu.VMEM((2, tiles // 2, rows, LANES), bf16),
            pltpu.VMEM((STEPS + 1, 2, tiles // 2, rows, LANES), bf16),
            pltpu.VMEM((orbs, tiles, ext, LANES), f32),
            pltpu.VMEM((orbs, 3, tiles, ext, LANES), f32),
            pltpu.VMEM((tiles, ext, LANES), f32),
            pltpu.VMEM((tiles, planes, LANES), f32),
            pltpu.VMEM((orbs, tiles, ext + 16, LANES), f32),
            pltpu.VMEM((orbs, tiles + 2, ext, LANES), f32),
            pltpu.VMEM((orbs, tiles, ext, LANES), f32),
            pltpu.VMEM((orbs, tiles + 2, ext, LANES), f32),
            pltpu.SemaphoreType.DMA((1,)),
            pltpu.SemaphoreType.DMA((STEPS, orbs)),
            pltpu.SemaphoreType.DMA((STEPS, orbs)),
            pltpu.SemaphoreType.DMA((STEPS + 1, 2)),
            pltpu.SemaphoreType.DMA((STEPS + 1, 2)),
        ],
        compiler_params=pltpu.CompilerParams(collective_id=0, has_side_effects=True),
        name="exchange",
    )(orbitals, occ)


def solution(mesh):
    in_specs = (P("band", "slab", None), P("band"))
    out_specs = P("band", "slab", None)
    return jax.shard_map(
        functools.partial(per_device, mesh.shape["band"], mesh.shape["slab"]),
        mesh=mesh, in_specs=in_specs, out_specs=out_specs, check_vma=False,
    )
```

```python
import functools
import math

import jax
import jax.numpy as jnp
from jax import lax
from jax.experimental import pallas as pl
from jax.experimental.pallas import tpu as pltpu
from jax.sharding import PartitionSpec as P

NZ = 64
STEPS = 3
LANES = 128
WIDTH = 2
UNROLL = 8
MESH = pl.DeviceIdType.MESH


screening = 0.5
ratio_mid = (12.0 + 2.0 * screening) / 12.0
root_term = math.sqrt(ratio_mid * ratio_mid - 1.0)
decay_ratio = ratio_mid - root_term
coeff_zero = 1.0 / (6.0 * root_term)
coeff_one = -2.0 * decay_ratio * coeff_zero
coeff_two = 2.0 * decay_ratio * decay_ratio * coeff_zero

scale = coeff_two / 18.0
inner = -coeff_one / 6.0 / scale
outer = (coeff_zero - coeff_two) / scale


def loop(count, body, unroll=1):
    lax.fori_loop(0, count, lambda i, c: (body(i), c)[1], 0, unroll=unroll)


def lane_tile(t):
    return pl.ds(pl.multiple_of(t * LANES, LANES), LANES)


def kernel(n_band, n_slab, orb_ref, occ_ref, out_ref, slots, edges, halos, own, own_moved, vis,
           weighted, dens, turned, part, inner_field, shifts, across, load_sem, send_sem, recv_sem, edge_send, edge_recv):
    orbs, planes, cells = orb_ref.shape
    tiles = cells // LANES
    ext = vis.shape[1]
    mine = STEPS
    band, slab = lax.axis_index("band"), lax.axis_index("slab")
    odd = lax.rem(band, 2)

    def at(by, side=0):
        return {"band": lax.rem(band + by + n_band, n_band), "slab": slab + side}

    sibling = at(1 - 2 * odd)
    has = (slab > 0, slab < n_slab - 1)
    step_of = (-1, 1)
    reach = {mine: 0, 1: 2, 0: 1 + 2 * odd}
    source = {mine: 0, 1: -2, 0: 2 * odd - 3}

    load = pltpu.make_async_copy(orb_ref, slots.at[mine, :, :, :cells], load_sem.at[0])
    load.start()

    barrier = pltpu.get_barrier_semaphore()
    for by in (source[1], source[0]):
        pl.semaphore_signal(barrier, inc=1, device_id=at(by), device_id_type=MESH)
    pl.semaphore_signal(barrier, inc=1, device_id=sibling, device_id_type=MESH)
    for side in range(2):
        @pl.when(has[side])
        def _(side=side):
            for slot in (mine, 1, 0):
                pl.semaphore_signal(barrier, inc=1, device_id=at(source[slot], step_of[side]), device_id_type=MESH)

    load.wait()
    for o in range(orbs):
        value = jnp.broadcast_to(occ_ref[:, o:o + 1].astype(jnp.float32), (planes, LANES))
        slots[mine, o, :, cells:] = value.astype(jnp.bfloat16)

    def cut(k):
        parts = ([], [])
        for h in range(2):
            for o in range(orbs):
                tile = slots[mine, o, :, lane_tile(2 * k + h)].astype(jnp.float32)
                parts[0].append(tile[:WIDTH])
                parts[1].append(tile[planes - WIDTH:])
        for side in range(2):
            edges[side, k] = jnp.concatenate(parts[side], axis=0).astype(jnp.bfloat16)

    loop(tiles // 2, cut, 2)

    for side in range(2):
        @pl.when(jnp.logical_not(has[side]))
        def _(side=side):
            halos[:, side] = jnp.zeros(halos.shape[:1] + halos.shape[2:], jnp.bfloat16)

    sides = has[0].astype(jnp.int32) + has[1].astype(jnp.int32)
    pl.semaphore_wait(barrier, 3 + 3 * sides)

    def edge_copy(side, slot):
        return pltpu.make_async_remote_copy(
            src_ref=edges.at[side], dst_ref=halos.at[slot, 1 - side],
            send_sem=edge_send.at[slot, side], recv_sem=edge_recv.at[slot, 1 - side],
            device_id=at(reach[slot], step_of[side]), device_id_type=MESH)

    def edge_pass(side):
        return pltpu.make_async_remote_copy(
            src_ref=halos.at[1, side], dst_ref=halos.at[2, side],
            send_sem=edge_send.at[2, side], recv_sem=edge_recv.at[2, side],
            device_id=sibling, device_id_type=MESH)

    def edge_wait(side, slot):
        pltpu.make_async_remote_copy(
            src_ref=edges.at[1 - side], dst_ref=halos.at[slot, side],
            send_sem=edge_send.at[slot, 1 - side], recv_sem=edge_recv.at[slot, side],
            device_id=sibling, device_id_type=MESH).wait_recv()

    def block_copy(slot, o):
        return pltpu.make_async_remote_copy(
            src_ref=slots.at[mine, o], dst_ref=slots.at[slot, o], send_sem=send_sem.at[slot, o],
            recv_sem=recv_sem.at[slot, o], device_id=at(reach[slot]), device_id_type=MESH)

    def block_pass(o):
        return pltpu.make_async_remote_copy(
            src_ref=slots.at[1, o], dst_ref=slots.at[2, o], send_sem=send_sem.at[2, o],
            recv_sem=recv_sem.at[2, o], device_id=sibling, device_id_type=MESH)

    def each_side(action):
        for side in range(2):
            pl.when(has[side])(functools.partial(action, side))

    each_side(lambda side: edge_copy(side, mine).start())
    each_side(lambda side: edge_copy(side, 1).start())
    each_side(lambda side: edge_copy(side, 0).start())
    for o in range(orbs):
        block_copy(1, o).start()
        block_copy(0, o).start()

    for i in range(orbs):
        for t in (0, tiles + 1):
            turned[i, t] = jnp.zeros(turned.shape[2:], jnp.float32)
            inner_field[i, t] = jnp.zeros(inner_field.shape[2:], jnp.float32)

    high = lax.broadcasted_iota(jnp.int32, (1, LANES), 1) >= NZ
    row = lax.broadcasted_iota(jnp.int32, (ext, LANES), 0)
    below = jnp.where(has[0], 1.0, 0.0)
    above = jnp.where(has[1], 1.0, 0.0)
    row_mask = jnp.where(row == WIDTH - 1, below, jnp.where(row == planes + WIDTH, above, 1.0))

    def ones(cond):
        return jnp.where(cond, 1.0, 0.0)

    src = lax.broadcasted_iota(jnp.int32, (LANES, LANES), 0)
    dst_lane = lax.broadcasted_iota(jnp.int32, (LANES, LANES), 1)
    swap = ones(src == (dst_lane + NZ) % LANES)
    left = jnp.where(dst_lane % NZ == 0, 0.0, ones(src == dst_lane - 1))
    right = jnp.where(dst_lane % NZ == NZ - 1, 0.0, ones(src == dst_lane + 1))
    for n, matrix in enumerate((swap, left, right)):
        shifts[:, n * LANES:(n + 1) * LANES] = matrix.astype(jnp.bfloat16)
    across[:LANES] = (swap + left + right).astype(jnp.bfloat16)
    across[LANES:] = swap.astype(jnp.bfloat16)

    def moves(tile_rows):
        return jnp.dot(tile_rows.astype(jnp.bfloat16), shifts[...], preferred_element_type=jnp.float32)

    def pick(rows, h, o):
        value = None
        for q in range(orbs):
            r = (h * orbs + q) * WIDTH
            piece = rows[r:r + WIDTH]
            value = piece if value is None else jnp.where(o == q, piece, value)
        return value

    def widen(slot, o, dst):
        def body(k):
            low = halos[slot, 0, k].astype(jnp.float32)
            up = halos[slot, 1, k].astype(jnp.float32)
            for h in range(2):
                t = 2 * k + h
                dst[t, :WIDTH] = pick(low, h, o)
                dst[t, planes + WIDTH:planes + 2 * WIDTH] = pick(up, h, o)
                dst[t, WIDTH:planes + WIDTH] = slots[slot, o, :, lane_tile(t)].astype(jnp.float32)
        loop(tiles // 2, body, 4)

    def visit(slot, o):
        weight = -scale * slots[slot, o, :, cells:].astype(jnp.float32)
        widen(slot, o, vis)

        def density(k):
            both = jnp.concatenate([vis[2 * k], vis[2 * k + 1]], axis=0)
            moved = moves(both)
            for h in range(2):
                t = 2 * k + h
                mid = both[h * ext:(h + 1) * ext]
                turn_v, left_v, right_v = [
                    moved[h * ext:(h + 1) * ext, n * LANES:(n + 1) * LANES] for n in range(3)]
                weighted[t] = weight * vis[t, WIDTH:planes + WIDTH]
                for i in range(orbs):
                    d = own[i, t] * mid
                    dens[i, t, 8:ext + 8] = d
                    turn = own_moved[i, 0, t] * turn_v
                    turned[i, t + 1] = turn
                    part[i, t] = inner * d + turn + (own_moved[i, 1, t] * left_v + own_moved[i, 2, t] * right_v)

        def once(t):
            for i in range(orbs):
                along = dens[i, t, 7:ext + 7] + dens[i, t, 9:ext + 9]
                u = part[i, t] + along + jnp.where(high, turned[i, t + 2], turned[i, t])
                inner_field[i, t + 1] = u * row_mask

        def twice(t):
            rows = slice(WIDTH, planes + WIDTH)
            field = jnp.concatenate([
                jnp.concatenate([inner_field[i, t + 1, rows] for i in range(orbs)], axis=0),
                jnp.concatenate([
                    jnp.where(high, inner_field[i, t, rows], inner_field[i, t + 2, rows])
                    for i in range(orbs)], axis=0)], axis=1)
            top = field.astype(jnp.bfloat16)
            rest = (field - top.astype(jnp.float32)).astype(jnp.bfloat16)
            matrix = across[...]
            plane_sum = jnp.dot(top, matrix, preferred_element_type=jnp.float32)
            plane_sum = plane_sum + jnp.dot(rest, matrix, preferred_element_type=jnp.float32)
            for i in range(orbs):
                v = inner_field[i, t + 1, WIDTH - 1:planes + WIDTH - 1] + inner_field[i, t + 1, WIDTH + 1:planes + WIDTH + 1]
                v = v + plane_sum[i * planes:(i + 1) * planes]
                v = v + outer * dens[i, t, 8 + WIDTH:8 + planes + WIDTH]
                out_ref[i, :, lane_tile(t)] += weighted[t] * v

        loop(tiles // 2, density, UNROLL // 2)
        loop(tiles, once, UNROLL)
        loop(tiles, twice, UNROLL)

    each_side(lambda side: edge_wait(side, mine))
    for i in range(orbs):
        widen(mine, i, own.at[i])

    def prepare(t):
        for i in range(orbs):
            moved = moves(own[i, t])
            for n in range(3):
                own_moved[i, n, t] = moved[:, n * LANES:(n + 1) * LANES]
            out_ref[i, :, lane_tile(t)] = jnp.zeros((planes, LANES), jnp.float32)

    loop(tiles, prepare, UNROLL)

    if_odd, if_even = [(mine, o) for o in range(orbs)], [(mine, o) for o in range(orbs)]
    if_odd += [(0, o) for o in range(orbs)]
    for o in range(orbs):
        if_odd += [(1, o), (2, o)]
        if_even += [(1, o), (0, o), (2, o)]

    def entry(k, column):
        value = jnp.int32(0)
        for n, (a, b) in enumerate(zip(if_odd, if_even)):
            value = jnp.where(k == n, jnp.where(odd == 1, a[column], b[column]), value)
        return value

    def step(k):
        slot, o = entry(k, 0), entry(k, 1)
        for q in range(STEPS):
            for p in range(orbs):
                @pl.when(jnp.logical_and(slot == q, o == p))
                def _(q=q, p=p):
                    if p == 0:
                        each_side(lambda side: edge_wait(side, q))
                        if q == 1:
                            each_side(lambda side: edge_pass(side).start())
                    (block_pass(p) if q == 2 else block_copy(q, p)).wait_recv()
                    if q == 1:
                        block_pass(p).start()
        visit(slot, o)

    loop(len(if_odd), step)

    for o in range(orbs):
        block_copy(0, o).wait_send()
        block_copy(1, o).wait_send()
        block_pass(o).wait_send()
    for slot in (mine, 1, 0):
        each_side(lambda side: edge_copy(side, slot).wait_send())
    each_side(lambda side: edge_pass(side).wait_send())


def per_device(n_band, n_slab, orbitals, occupation):
    orbs, planes, cells = orbitals.shape
    tiles = cells // LANES
    ext = -(-(planes + 2 * WIDTH) // 8) * 8
    occ = occupation.reshape(1, orbs)
    f32, bf16 = jnp.float32, jnp.bfloat16
    rows = 2 * orbs * WIDTH
    return pl.pallas_call(
        functools.partial(kernel, n_band, n_slab),
        out_shape=jax.ShapeDtypeStruct(orbitals.shape, f32),
        in_specs=[pl.BlockSpec(memory_space=pl.ANY), pl.BlockSpec(memory_space=pltpu.VMEM)],
        out_specs=pl.BlockSpec(memory_space=pltpu.VMEM),
        scratch_shapes=[
            pltpu.VMEM((STEPS + 1, orbs, planes, cells + LANES), bf16),
            pltpu.VMEM((2, tiles // 2, rows, LANES), bf16),
            pltpu.VMEM((STEPS + 1, 2, tiles // 2, rows, LANES), bf16),
            pltpu.VMEM((orbs, tiles, ext, LANES), f32),
            pltpu.VMEM((orbs, 3, tiles, ext, LANES), f32),
            pltpu.VMEM((tiles, ext, LANES), f32),
            pltpu.VMEM((tiles, planes, LANES), f32),
            pltpu.VMEM((orbs, tiles, ext + 16, LANES), f32),
            pltpu.VMEM((orbs, tiles + 2, ext, LANES), f32),
            pltpu.VMEM((orbs, tiles, ext, LANES), f32),
            pltpu.VMEM((orbs, tiles + 2, ext, LANES), f32),
            pltpu.VMEM((LANES, 3 * LANES), bf16),
            pltpu.VMEM((2 * LANES, LANES), bf16),
            pltpu.SemaphoreType.DMA((1,)),
            pltpu.SemaphoreType.DMA((STEPS, orbs)),
            pltpu.SemaphoreType.DMA((STEPS, orbs)),
            pltpu.SemaphoreType.DMA((STEPS + 1, 2)),
            pltpu.SemaphoreType.DMA((STEPS + 1, 2)),
        ],
        compiler_params=pltpu.CompilerParams(collective_id=0, has_side_effects=True),
        name="exchange",
    )(orbitals, occ)


def solution(mesh):
    in_specs = (P("band", "slab", None), P("band"))
    out_specs = P("band", "slab", None)
    return jax.shard_map(
        functools.partial(per_device, mesh.shape["band"], mesh.shape["slab"]),
        mesh=mesh, in_specs=in_specs, out_specs=out_specs, check_vma=False,
    )
```
